32 devices in a mesh: gx: 4 (over y, x), gy: 4 (over z), gz: 2 (over core).
Axes of the slice: x: 2, y: 2, z: 4, core: 2. Of those that a mesh axis runs over, the one named last changes fastest.
Arguments:
- fields: bfloat16 [4096, 2048], P(('gx', 'gy', 'gz')), may hold values from -6 to 6
- coordinates: float32 [3, 524288], P(None, ('gx', 'gy', 'gz')), may hold values from -1 to 1
- element_rank: int32 [524288, 1], P(('gx', 'gy', 'gz')), may hold values from 0 to 31; in each aligned block of 16384 rows (0 to 16383, 16384 to 32767, ...) at most 640 rows name the same one
- element_slot: int32 [524288], P(('gx', 'gy', 'gz')), may hold values from 0 to 127
Outputs:
- samples: float32 [4, 524288], P(None, ('gx', 'gy', 'gz'))
The draws below stay inside these ranges and needn't reach their ends.
Inputs may be any that keep to these rules, and one draw needn't show every extreme that they name: `element_rank`: among the probes of one device no rank is named by more than 640 probes, and in some devices' blocks one rank is named by exactly 640.
All inputs are finite; a program needn't handle non-finite values.
Results may differ from the reference program's by a relative error of at most 0.0024.
Values sent between devices are 32-bit elements; how exact they have to be, the bound alone decides.
A program may use at most 64 MiB of HBM per device.

```python
import math
import jax
import jax.numpy as jnp
import numpy as np
from jax import lax

ROW = 2048
E_DEV = 128
P_DEV = 16384
CAP = 640
ELEMENTS = 4096
PROBES = 524288
DEVICES = 32


def place_ends(values, key, least, largest):
    longest = values.shape.index(max(values.shape))
    spots = []
    for shift in (0, 1):
        where = [jax.random.randint(jax.random.fold_in(key, axis), (), 0, length) for axis, length in enumerate(values.shape)]
        where[longest] = (where[longest] + shift) % values.shape[longest]
        spots.append(tuple(where))
    return values.at[spots[0]].set(least).at[spots[1]].set(largest)


def shard_levels(rng, dims, split, least, largest):
    loudness = 1.0
    for axis_at, parts in split:
        heights = jax.random.uniform(jax.random.fold_in(jax.random.fold_in(rng, 6), axis_at), (parts,), jnp.float32, least / len(split), largest / len(split))
        loudness = loudness * jnp.repeat(jnp.exp(heights), dims[axis_at] // parts).reshape((-1,) + (1,) * (len(dims) - 1 - axis_at))
    return loudness


def routed_block(key, own, number, rows, count, top, most, slope):
    sequence = jax.random.permutation(key, count)
    packed, usual = shares(count, rows * top, most, slope, True), shares(count, rows * top, most, slope, False)
    places = jnp.arange(count)

    def named(sizes, turn):
        used = int((sizes > 0).sum())
        fixed = max(1, used // 4)
        shifted = fixed + (places - fixed + turn * (used - fixed)) % max(1, count - fixed)
        return jnp.zeros((count,), jnp.int32).at[sequence[jnp.where(places < fixed, places, shifted)]].set(jnp.asarray(sizes, jnp.int32))

    sizes = jnp.where(number % 4 == 0, named(packed, number // 4), named(usual, number - number // 4 - 1))
    mixed = jax.random.permutation(jax.random.fold_in(own, 3), count)
    source_of, sink = mixed[0:count // 2 * 2:2], mixed[1:count // 2 * 2:2]
    margin = jnp.minimum(sizes[source_of] - 1, most - sizes[sink]) // 2
    margin = jnp.where((source_of == sequence[0]) | (sink == sequence[0]) | (sizes[sink] == 0), 0, jnp.maximum(margin, 0))
    shifted = jax.random.randint(jax.random.fold_in(own, 4), (count // 2,), 0, 1 << 20) % (margin + 1)
    sizes = sizes.at[source_of].add(-shifted).at[sink].add(shifted)
    labels = jnp.searchsorted(jnp.cumsum(sizes), jnp.arange(rows * top), side="right").astype(jnp.int32)
    listing = labels.reshape(top, rows).T
    listing = listing[jax.random.permutation(jax.random.fold_in(own, 1), rows)]
    turn = jax.random.randint(jax.random.fold_in(own, 2), (rows, 1), 0, top)
    return jnp.take_along_axis(listing, (jnp.arange(top)[None, :] + turn) % top, axis=1)


def shares(count, total, bound, skew, full):
    loads = [(1 << 20) // math.isqrt(standing ** skew) + 1 for standing in range(1, count + 1)]
    largest = bound if full else min(bound, max(-(-total // count), total * loads[0] // sum(loads)))
    least = 1 if total - largest >= count - 1 else 0
    given, rest = [largest] + [least] * (count - 1), total - largest - least * (count - 1)
    while rest > 0:
        free = [i for i in range(1, count) if given[i] < largest] or [i for i in range(1, count) if given[i] < bound]
        pool, remaining = sum([loads[i] for i in free]), rest
        for i in free:
            addition = min(bound - given[i], max(1, remaining * loads[i] // pool), rest)
            given[i] = given[i] + addition
            rest = rest - addition
    return np.array(given)


def bell_draw(own_key, extent, spread, most, shards=(), held_as=jnp.bfloat16):
    drawn = jax.random.normal(own_key, extent, jnp.float32) * spread
    if len(shards) > 0:
        drawn = shard_levels(own_key, extent, shards, -0.22, 0.18) * drawn
    return jnp.clip(drawn, min=-most, max=most).astype(held_as)


def setup_inputs(seed: int = 0) -> dict:
    arg_keys = jax.random.split(jax.random.key(seed), 5)
    fields = bell_draw(arg_keys[0], (ELEMENTS, ROW), 1.0, 6.0, ((0, 32),))
    coordinates = jnp.clip(jax.random.uniform(arg_keys[1], (3, PROBES), jnp.float32, -1.0, 1.0) * shard_levels(arg_keys[1], (3, PROBES), ((1, 32),), -0.4, 0.0), -1.0, 1.0)
    element_rank_keys = jax.random.split(jax.random.fold_in(arg_keys[2], 1), PROBES // P_DEV)
    element_rank_turns = jax.random.permutation(jax.random.fold_in(arg_keys[2], 3), PROBES // P_DEV)
    element_rank = jax.vmap(lambda own, number: routed_block(jax.random.fold_in(arg_keys[2], 2), own, number, P_DEV, DEVICES, 1, CAP, 2))(element_rank_keys, element_rank_turns).reshape((PROBES, 1))
    element_slot = place_ends(jax.random.randint(arg_keys[3], (PROBES,), 0, E_DEV), jax.random.fold_in(arg_keys[3], 1), 0, E_DEV - 1).astype(jnp.int32)
    return {"fields": fields, "coordinates": coordinates, "element_rank": element_rank, "element_slot": element_slot}


gll_points = np.array([-1.0, -0.8717401485096066, -0.5917001814331423, -0.2092992179024789, 0.2092992179024789, 0.5917001814331423, 0.8717401485096066, 1.0])
gll_scale = np.array([1.0 / np.prod([gll_points[a] - gll_points[b] for b in range(8) if b != a]) for a in range(8)])


def lagrange(coord):
    offsets = coord[None, :] - jnp.asarray(gll_points, coord.dtype)[:, None]
    weights = []
    for node_a in range(8):
        factor = jnp.ones_like(coord) * gll_scale[node_a]
        for node_b in range(8):
            if node_b != node_a:
                factor = factor * offsets[node_b]
        weights.append(factor)
    return jnp.stack(weights, axis=0)


def interpolate(coordinates, element, fields):
    total_rows = element.shape[0]
    block_rows = math.gcd(total_rows, 8192)
    block_count = total_rows // block_rows

    def one_block(pieces):
        coords_block, slots_block = pieces
        weight_r = lagrange(coords_block[0])
        weight_s = lagrange(coords_block[1])
        weight_t = lagrange(coords_block[2]).astype(jnp.bfloat16)
        gathered = jnp.take(fields, slots_block, axis=0).reshape(block_rows, 256, 8)
        along_t = jnp.einsum("nak,kn->na", gathered.astype(jnp.float32), weight_t.astype(jnp.float32), precision=lax.Precision.HIGHEST)
        along_t = along_t.reshape(block_rows, 4, 8, 8)
        along_s = jnp.einsum("nfij,jn->nfi", along_t, weight_s, precision=lax.Precision.HIGHEST)
        return jnp.einsum("nfi,in->fn", along_s, weight_r, precision=lax.Precision.HIGHEST)

    coords_blocks = coordinates.reshape(3, block_count, block_rows).transpose(1, 0, 2)
    slot_blocks = element.reshape(block_count, block_rows)
    result = lax.map(one_block, (coords_blocks, slot_blocks))
    return result.transpose(1, 0, 2).reshape(4, total_rows)


def reference(fields, coordinates, element_rank, element_slot):
    element = element_rank[:, 0].astype(jnp.int32) * E_DEV + element_slot.astype(jnp.int32)
    return interpolate(coordinates, element, fields)
```

```python
import functools

import jax
import jax.numpy as jnp
import numpy as np
from jax import lax
from jax.experimental import pallas as pl
from jax.experimental.pallas import tpu as pltpu
from jax.sharding import PartitionSpec as P

AXES = ("gx", "gy", "gz")
F32, BF16 = jnp.float32, jnp.bfloat16
LANES = 128
CHUNK = 256
ROWS_PER_DOT = 4

gll_points = np.array(
    [
        -1.0,
        -0.8717401485096066,
        -0.5917001814331423,
        -0.2092992179024789,
        0.2092992179024789,
        0.5917001814331423,
        0.8717401485096066,
        1.0,
    ]
)
gll_scale = np.array(
    [1.0 / np.prod([gll_points[a] - gll_points[b] for b in range(8) if b != a]) for a in range(8)]
)
node_table = np.stack(
    [gll_scale] + [np.roll(gll_points, -k) for k in range(1, 8)], axis=0
).reshape(64, 1)


def iota_bf16(shape):
    return lax.broadcasted_iota(jnp.int32, shape, 0).astype(F32).astype(BF16)


def spread(row, count):
    return jnp.broadcast_to(row, (count, row.shape[1])).astype(BF16)


def route_kernel(count, blocks, rank_ref, coords_ref, slot_ref, prefix_ref, send_ref, row_ref, lane_ref, acc_ref):
    probes = rank_ref.shape[1]
    group = max(1, CHUNK // count)
    targets = lax.broadcasted_iota(jnp.int32, (count, CHUNK), 0)

    def place(step, carry):
        masks, hots, ranks = [], [], []
        for g in range(group):
            at = pl.ds(pl.multiple_of((step * group + g) * CHUNK, CHUNK), CHUNK)
            rank = rank_ref[:, at]
            mask = targets == jnp.broadcast_to(rank, (count, CHUNK))
            masks.append(mask)
            hots.append(jnp.where(mask, 1.0, 0.0).astype(BF16))
            ranks.append(rank.astype(F32))
        counted = jnp.dot(jnp.concatenate(hots, axis=0), prefix_ref[...], preferred_element_type=F32)
        for g in range(group):
            at = pl.ds(pl.multiple_of((step * group + g) * CHUNK, CHUNK), CHUNK)
            piece = counted[g * count : (g + 1) * count]
            place_in = jnp.where(masks[g], piece[:, :CHUNK] + carry, 0.0)
            position = jnp.sum(place_in, axis=0, keepdims=True) - 1.0
            block = jnp.floor(position * (1.0 / LANES))
            lane_ref[:, at] = position - block * LANES
            row_ref[:, at] = block * count + ranks[g]
            carry = carry + piece[:, CHUNK:]
        return carry

    lax.fori_loop(0, probes // (CHUNK * group), place, jnp.zeros((count, CHUNK), F32))

    rows = count * blocks
    row_ids = iota_bf16((rows, CHUNK))
    lane_ids = iota_bf16((LANES, CHUNK))
    acc_ref[...] = jnp.zeros_like(acc_ref)

    def scatter(step, _):
        row_hots, lane_parts = [], []
        for g in range(4):
            at = pl.ds(pl.multiple_of((step * 4 + g) * CHUNK, CHUNK), CHUNK)
            row_hots.append(
                jnp.where(row_ids == spread(row_ref[:, at], rows), jnp.ones((), BF16), jnp.zeros((), BF16))
            )
            here = lane_ids == spread(lane_ref[:, at], LANES)
            parts = []
            for v in range(3):
                value = coords_ref[v : v + 1, at]
                high = value.astype(BF16).astype(F32)
                parts += [high, value - high]
            parts.append(slot_ref[:, at].astype(F32))
            lane_parts.append(
                jnp.concatenate(
                    [jnp.where(here, spread(part, LANES), jnp.zeros((), BF16)) for part in parts], axis=0
                )
            )
        acc_ref[...] += lax.dot_general(
            jnp.concatenate(row_hots, axis=1),
            jnp.concatenate(lane_parts, axis=1),
            (((1,), (1,)), ((), ())),
            preferred_element_type=F32,
        )
        return 0

    lax.fori_loop(0, probes // (4 * CHUNK), scatter, 0)
    for b in range(blocks):
        at = slice(b * count, (b + 1) * count)
        for v in range(3):
            high = acc_ref[at, 2 * v * LANES : (2 * v + 1) * LANES]
            low = acc_ref[at, (2 * v + 1) * LANES : (2 * v + 2) * LANES]
            send_ref[v * blocks + b] = high + low
        send_ref[3 * blocks + b] = acc_ref[at, 6 * LANES : 7 * LANES]


def exchange_kernel(sizes, send_ref, recv_ref, send_sem, recv_sem, own_sem):
    count = sizes[0] * sizes[1] * sizes[2]
    me = (lax.axis_index("gx") * sizes[1] + lax.axis_index("gy")) * sizes[2] + lax.axis_index("gz")

    def coordinates_of(device):
        return (device // (sizes[1] * sizes[2]), (device // sizes[2]) % sizes[1], device % sizes[2])

    barrier = pltpu.get_barrier_semaphore()

    def greet(step, _):
        other = lax.rem(me + step, count)
        pl.semaphore_signal(
            barrier, inc=1, device_id=coordinates_of(other), device_id_type=pl.DeviceIdType.MESH
        )
        return 0

    lax.fori_loop(1, count, greet, 0)
    own = pltpu.make_async_copy(send_ref.at[:, me], recv_ref.at[:, me], own_sem)
    own.start()
    pl.semaphore_wait(barrier, count - 1)

    def copy_to(step):
        other = lax.rem(me + step, count)
        return pltpu.make_async_remote_copy(
            src_ref=send_ref.at[:, other],
            dst_ref=recv_ref.at[:, me],
            send_sem=send_sem.at[step],
            recv_sem=recv_sem.at[step],
            device_id=coordinates_of(other),
            device_id_type=pl.DeviceIdType.MESH,
        )

    def begin(step, _):
        copy_to(step).start()
        return 0

    lax.fori_loop(1, count, begin, 0)

    def finish(step, _):
        copy_to(step).wait()
        return 0

    lax.fori_loop(1, count, finish, 0)
    own.wait()


def lagrange(coord, nodes_ref):
    weight = nodes_ref[0:8, :]
    spread_coord = jnp.broadcast_to(coord, (8, LANES))
    for k in range(1, 8):
        weight = weight * (spread_coord - nodes_ref[8 * k : 8 * k + 8, :])
    return weight


def interpolate_kernel(blocks, recv_ref, fields_ref, nodes_ref, values_ref, picker_ref):
    count = recv_ref.shape[1]
    depth = fields_ref.shape[1]
    elements = depth // 8
    per_block = count // ROWS_PER_DOT
    zero = jnp.zeros((), BF16)
    ids = iota_bf16((16, LANES))

    def half(step, buffer):
        block = step // per_block
        first = (step % per_block) * ROWS_PER_DOT
        weights = []
        for j in range(ROWS_PER_DOT):
            r, s, t, slot = [recv_ref[v * blocks + block, pl.ds(first + j, 1), :] for v in range(4)]
            weights.append((lagrange(r, nodes_ref), lagrange(s, nodes_ref)))
            weight_t = lagrange(t, nodes_ref)
            columns = slice(j * LANES, (j + 1) * LANES)
            masks = [ids == spread(slot - float(16 * k), 16) for k in range(elements // 16)]
            for c in range(8):
                weight = spread(weight_t[c : c + 1, :], 16)
                for k in range(elements // 16):
                    at = c * elements + k * 16
                    picker_ref[buffer, at : at + 16, columns] = jnp.where(masks[k], weight, zero)
        along = jnp.dot(fields_ref[...], picker_ref[buffer], preferred_element_type=F32)
        for j in range(ROWS_PER_DOT):
            weight_r, weight_s = weights[j]
            columns = slice(j * LANES, (j + 1) * LANES)
            factors = [jnp.broadcast_to(weight_r[a : a + 1, :], (8, LANES)) for a in range(8)]
            for f in range(4):
                total = along[f * 64 : f * 64 + 8, columns] * factors[0]
                for a in range(1, 8):
                    total += along[f * 64 + a * 8 : f * 64 + a * 8 + 8, columns] * factors[a]
                values_ref[f * blocks + block, pl.ds(first + j, 1), :] = jnp.sum(
                    total * weight_s, axis=0, keepdims=True
                )

    def body(step, _):
        half(step * 2, 0)
        half(step * 2 + 1, 1)
        return 0

    lax.fori_loop(0, blocks * per_block // 2, body, 0)


def return_kernel(blocks, values_ref, row_ref, lane_ref, out_ref, table_ref):
    probes = row_ref.shape[1]
    count = values_ref.shape[1]
    rows = blocks * count
    for f in range(4):
        table = jnp.concatenate([values_ref[f * blocks + b] for b in range(blocks)], axis=0)
        table_ref[f * LANES : (f + 1) * LANES, :] = table.T.astype(BF16)
    row_ids = iota_bf16((rows, CHUNK))
    lane_ids = lax.broadcasted_iota(jnp.int32, (LANES, CHUNK), 0).astype(F32)

    def body(step, _):
        for g in range(2):
            at = pl.ds(pl.multiple_of((step * 2 + g) * CHUNK, CHUNK), CHUNK)
            hot = jnp.where(row_ids == spread(row_ref[:, at], rows), jnp.ones((), BF16), jnp.zeros((), BF16))
            picked = jnp.dot(table_ref[...], hot, preferred_element_type=F32)
            here = lane_ids == jnp.broadcast_to(lane_ref[:, at], (LANES, CHUNK))
            for f in range(4):
                out_ref[f : f + 1, at] = jnp.sum(
                    jnp.where(here, picked[f * LANES : (f + 1) * LANES], 0.0), axis=0, keepdims=True
                )
        return 0

    lax.fori_loop(0, probes // (2 * CHUNK), body, 0)


VMEM = pl.BlockSpec(memory_space=pltpu.VMEM)


def call(kernel, inputs, outputs, scratch, **options):
    return pl.pallas_call(
        kernel,
        out_shape=outputs,
        in_specs=[VMEM] * inputs,
        out_specs=jax.tree.map(lambda _: VMEM, outputs),
        scratch_shapes=scratch,
        compiler_params=pltpu.CompilerParams(vmem_limit_bytes=48 << 20, **options),
    )


def exchange(sizes, array, number):
    count = array.shape[1]
    return call(
        functools.partial(exchange_kernel, sizes),
        1,
        jax.ShapeDtypeStruct(array.shape, F32),
        [
            pltpu.SemaphoreType.DMA((count,)),
            pltpu.SemaphoreType.DMA((count,)),
            pltpu.SemaphoreType.DMA,
        ],
        collective_id=number,
        has_side_effects=True,
    )(array)


def local(sizes, fields, coordinates, element_rank, element_slot):
    count = sizes[0] * sizes[1] * sizes[2]
    probes = element_slot.shape[0]
    elements = fields.shape[0]
    capacity = 5 * probes // (4 * count)
    blocks = -(-capacity // LANES)
    layout = jax.ShapeDtypeStruct((4 * blocks, count, LANES), F32)
    line = jax.ShapeDtypeStruct((1, probes), F32)

    lower = np.arange(CHUNK)
    prefix = np.concatenate([lower[:, None] <= lower[None, :], np.ones((CHUNK, CHUNK))], axis=1)
    send, row, lane = call(
        functools.partial(route_kernel, count, blocks),
        4,
        (layout, line, line),
        [pltpu.VMEM((count * blocks, 7 * LANES), F32)],
    )(
        element_rank.reshape(1, probes),
        coordinates,
        element_slot.reshape(1, probes),
        jnp.asarray(prefix, BF16),
    )
    arrived = exchange(sizes, send, 0)
    turned = fields.reshape(elements, 256, 8).transpose(1, 2, 0).reshape(256, 8 * elements)
    nodes = jnp.broadcast_to(jnp.asarray(node_table, F32), (64, LANES))
    values = call(
        functools.partial(interpolate_kernel, blocks),
        3,
        layout,
        [pltpu.VMEM((2, 8 * elements, ROWS_PER_DOT * LANES), BF16)],
    )(arrived, turned, nodes)
    returned = exchange(sizes, values, 1)
    return call(
        functools.partial(return_kernel, blocks),
        3,
        jax.ShapeDtypeStruct((4, probes), F32),
        [pltpu.VMEM((4 * LANES, count * blocks), BF16)],
    )(returned, row, lane)


def solution(mesh):
    sizes = tuple(mesh.shape[axis] for axis in AXES)
    placed = (P(AXES, None), P(None, AXES), P(AXES, None), P(AXES))
    return jax.shard_map(
        functools.partial(local, sizes),
        mesh=mesh,
        in_specs=placed,
        out_specs=P(None, AXES),
        check_vma=False,
    )
```

```python
import functools

import jax
import jax.numpy as jnp
import numpy as np
from jax import lax
from jax.experimental import pallas as pl
from jax.experimental.pallas import tpu as pltpu
from jax.sharding import PartitionSpec as P

AXES = ("gx", "gy", "gz")
F32, BF16 = jnp.float32, jnp.bfloat16
LANES = 128
CHUNK = 256
GROUP = 4

gll_points = np.array(
    [
        -1.0,
        -0.8717401485096066,
        -0.5917001814331423,
        -0.2092992179024789,
        0.2092992179024789,
        0.5917001814331423,
        0.8717401485096066,
        1.0,
    ]
)
gll_scale = np.array(
    [1.0 / np.prod([gll_points[a] - gll_points[b] for b in range(8) if b != a]) for a in range(8)]
)
node_table = np.stack(
    [gll_scale] + [np.roll(gll_points, -k) for k in range(1, 8)], axis=0
).reshape(64, 1)


def iota_bf16(shape):
    return lax.broadcasted_iota(jnp.int32, shape, 0).astype(F32).astype(BF16)


def spread(row, count):
    return jnp.broadcast_to(row, (count, row.shape[1])).astype(BF16)


def route(count, blocks, rank_ref, coords_ref, slot_ref, prefix_ref, send_ref, row_ref, lane_ref, acc_ref):
    probes = rank_ref.shape[1]
    group = max(1, CHUNK // count)
    targets = lax.broadcasted_iota(jnp.int32, (count, CHUNK), 0)

    def place(step, carry):
        masks, hots, ranks = [], [], []
        for g in range(group):
            at = pl.ds(pl.multiple_of((step * group + g) * CHUNK, CHUNK), CHUNK)
            rank = rank_ref[:, at]
            mask = targets == jnp.broadcast_to(rank, (count, CHUNK))
            masks.append(mask)
            hots.append(jnp.where(mask, 1.0, 0.0).astype(BF16))
            ranks.append(rank.astype(F32))
        counted = jnp.dot(jnp.concatenate(hots, axis=0), prefix_ref[...], preferred_element_type=F32)
        for g in range(group):
            at = pl.ds(pl.multiple_of((step * group + g) * CHUNK, CHUNK), CHUNK)
            piece = counted[g * count : (g + 1) * count]
            place_in = jnp.where(masks[g], piece[:, :CHUNK] + carry, 0.0)
            position = jnp.sum(place_in, axis=0, keepdims=True) - 1.0
            block = jnp.floor(position * (1.0 / LANES))
            lane_ref[:, at] = position - block * LANES
            row_ref[:, at] = block * count + ranks[g]
            carry = carry + piece[:, CHUNK:]
        return carry

    lax.fori_loop(0, probes // (CHUNK * group), place, jnp.zeros((count, CHUNK), F32))

    rows = count * blocks
    part_lanes = LANES // 2
    row_ids = iota_bf16((rows, CHUNK))
    lane_ids = iota_bf16((part_lanes, CHUNK))
    one, zero = jnp.ones((), BF16), jnp.zeros((), BF16)
    acc_ref[...] = jnp.zeros_like(acc_ref)

    def scatter(step, _):
        row_hots, lane_parts = [], []
        for g in range(4):
            at = pl.ds(pl.multiple_of((step * 4 + g) * CHUNK, CHUNK), CHUNK)
            row, lane = row_ref[:, at], lane_ref[:, at]
            upper = lane >= float(part_lanes)
            halves = [jnp.where(upper, -1.0, row), jnp.where(upper, row, -1.0)]
            row_hots.append(
                jnp.concatenate([jnp.where(row_ids == spread(part, rows), one, zero) for part in halves], axis=0)
            )
            here = lane_ids == spread(jnp.where(upper, lane - float(part_lanes), lane), part_lanes)
            parts = []
            for v in range(3):
                value = coords_ref[v : v + 1, at]
                high = value.astype(BF16).astype(F32)
                parts += [high, value - high]
            parts.append(slot_ref[:, at].astype(F32))
            chosen = [jnp.where(here, spread(part, part_lanes), zero) for part in parts]
            chosen.append(jnp.zeros((part_lanes, CHUNK), BF16))
            lane_parts.append(jnp.concatenate(chosen, axis=0))
        acc_ref[...] += lax.dot_general(
            jnp.concatenate(row_hots, axis=1),
            jnp.concatenate(lane_parts, axis=1),
            (((1,), (1,)), ((), ())),
            preferred_element_type=F32,
        )
        return 0

    lax.fori_loop(0, probes // (4 * CHUNK), scatter, 0)
    left = lax.broadcasted_iota(jnp.int32, (count, LANES), 1) < part_lanes
    for b in range(blocks):
        for v in range(4):
            sides = []
            for h in range(2):
                first = h * rows + b * count
                both = acc_ref[first : first + count, v * LANES : (v + 1) * LANES]
                sides.append(both + pltpu.roll(both, part_lanes, 1))
            send_ref[v * blocks + b] = jnp.where(left, sides[0], sides[1])


def lagrange(coord, nodes_ref):
    weight = nodes_ref[0:8, :]
    spread_coord = jnp.broadcast_to(coord, (8, LANES))
    for k in range(1, 8):
        weight = weight * (spread_coord - nodes_ref[8 * k : 8 * k + 8, :])
    return weight


def interpolate(blocks, block, sources, recv_ref, fields_ref, nodes_ref, values_ref, picker_ref):
    depth = fields_ref.shape[1]
    elements = depth // 8
    zero = jnp.zeros((), BF16)
    ids = iota_bf16((16, LANES))
    weights = []
    for j, source in enumerate(sources):
        r, s, t, slot = [recv_ref[v * blocks + block, pl.ds(source, 1), :] for v in range(4)]
        weights.append((lagrange(r, nodes_ref), lagrange(s, nodes_ref)))
        weight_t = lagrange(t, nodes_ref)
        columns = slice(j * LANES, (j + 1) * LANES)
        masks = [ids == spread(slot - float(16 * k), 16) for k in range(elements // 16)]
        for c in range(8):
            weight = spread(weight_t[c : c + 1, :], 16)
            for k in range(elements // 16):
                at = c * elements + k * 16
                picker_ref[at : at + 16, columns] = jnp.where(masks[k], weight, zero)
    along = jnp.dot(fields_ref[...], picker_ref[...], preferred_element_type=F32)
    for j, source in enumerate(sources):
        weight_r, weight_s = weights[j]
        columns = slice(j * LANES, (j + 1) * LANES)
        factors = [jnp.broadcast_to(weight_r[a : a + 1, :], (8, LANES)) for a in range(8)]
        for f in range(4):
            total = along[f * 64 : f * 64 + 8, columns] * factors[0]
            for a in range(1, 8):
                total += along[f * 64 + a * 8 : f * 64 + a * 8 + 8, columns] * factors[a]
            values_ref[f * blocks + block, pl.ds(source, 1), :] = jnp.sum(
                total * weight_s, axis=0, keepdims=True
            )


def sample_kernel(
    sizes,
    blocks,
    rank_ref,
    coords_ref,
    slot_ref,
    prefix_ref,
    fields_ref,
    nodes_ref,
    back_ref,
    row_ref,
    lane_ref,
    acc_ref,
    send_ref,
    recv_ref,
    values_ref,
    picker_even,
    picker_odd,
    out_sem,
    in_sem,
    back_out_sem,
    back_in_sem,
    own_sem,
):
    count = sizes[0] * sizes[1] * sizes[2]
    me = (lax.axis_index("gx") * sizes[1] + lax.axis_index("gy")) * sizes[2] + lax.axis_index("gz")
    mesh_ids = pl.DeviceIdType.MESH

    def coordinates_of(device):
        return (device // (sizes[1] * sizes[2]), (device // sizes[2]) % sizes[1], device % sizes[2])

    def each(first, last, act):
        def body(step, _):
            act(step)
            return 0

        lax.fori_loop(first, last, body, 0)

    def behind(step):
        return lax.rem(me + count - step, count)

    def outward(step):
        other = lax.rem(me + step, count)
        return pltpu.make_async_remote_copy(
            src_ref=send_ref.at[:, other],
            dst_ref=recv_ref.at[:, me],
            send_sem=out_sem.at[step],
            recv_sem=in_sem.at[step],
            device_id=coordinates_of(other),
            device_id_type=mesh_ids,
        )

    def backward(step):
        other = behind(step)
        return pltpu.make_async_remote_copy(
            src_ref=values_ref.at[:, other],
            dst_ref=back_ref.at[:, me],
            send_sem=back_out_sem.at[step],
            recv_sem=back_in_sem.at[step],
            device_id=coordinates_of(other),
            device_id_type=mesh_ids,
        )

    barrier = pltpu.get_barrier_semaphore()
    each(
        1,
        count,
        lambda step: pl.semaphore_signal(
            barrier, inc=1, device_id=coordinates_of(lax.rem(me + step, count)), device_id_type=mesh_ids
        ),
    )
    route(count, blocks, rank_ref, coords_ref, slot_ref, prefix_ref, send_ref, row_ref, lane_ref, acc_ref)
    pl.semaphore_wait(barrier, count - 1)
    each(1, count, lambda step: outward(step).start())
    own = pltpu.make_async_copy(send_ref.at[:, me], recv_ref.at[:, me], own_sem.at[0])
    own.start()
    own.wait()
    own_back = pltpu.make_async_copy(values_ref.at[:, me], back_ref.at[:, me], own_sem.at[1])
    pickers = [picker_even, picker_odd]

    def reply(group):
        for j in range(GROUP):
            step = group * GROUP + j
            if j == 0:

                @pl.when(step == 0)
                def _():
                    own_back.start()

                @pl.when(step > 0)
                def _():
                    backward(step).start()

            else:
                backward(step).start()

    def body(group, _):
        sources = []
        for j in range(GROUP):
            step = group * GROUP + j
            if j == 0:

                @pl.when(step > 0)
                def _():
                    outward(step).wait_recv()

            else:
                outward(step).wait_recv()
            sources.append(behind(step))
        for block in range(blocks):
            interpolate(blocks, block, sources, recv_ref, fields_ref, nodes_ref, values_ref, pickers[block % 2])

        @pl.when(group > 0)
        def _():
            reply(group - 1)

        return 0

    groups = count // GROUP
    lax.fori_loop(0, groups, body, 0)
    each(1, count, lambda step: outward(step).wait_send())
    reply(groups - 1)
    each(1, count, lambda step: backward(step).wait())
    own_back.wait()


def return_kernel(blocks, values_ref, row_ref, lane_ref, out_ref, table_ref):
    probes = row_ref.shape[1]
    count = values_ref.shape[1]
    rows = blocks * count
    for f in range(4):
        table = jnp.concatenate([values_ref[f * blocks + b] for b in range(blocks)], axis=0)
        table_ref[f * LANES : (f + 1) * LANES, :] = table.T.astype(BF16)
    row_ids = iota_bf16((rows, CHUNK))
    lane_ids = lax.broadcasted_iota(jnp.int32, (LANES, CHUNK), 0).astype(F32)

    def body(step, _):
        for g in range(4):
            at = pl.ds(pl.multiple_of((step * 4 + g) * CHUNK, CHUNK), CHUNK)
            hot = jnp.where(row_ids == spread(row_ref[:, at], rows), jnp.ones((), BF16), jnp.zeros((), BF16))
            picked = jnp.dot(table_ref[...], hot, preferred_element_type=F32)
            here = lane_ids == jnp.broadcast_to(lane_ref[:, at], (LANES, CHUNK))
            for f in range(4):
                out_ref[f : f + 1, at] = jnp.sum(
                    jnp.where(here, picked[f * LANES : (f + 1) * LANES], 0.0), axis=0, keepdims=True
                )
        return 0

    lax.fori_loop(0, probes // (4 * CHUNK), body, 0)


VMEM = pl.BlockSpec(memory_space=pltpu.VMEM)


def call(kernel, inputs, outputs, scratch, **options):
    return pl.pallas_call(
        kernel,
        out_shape=outputs,
        in_specs=[VMEM] * inputs,
        out_specs=jax.tree.map(lambda _: VMEM, outputs),
        scratch_shapes=scratch,
        compiler_params=pltpu.CompilerParams(vmem_limit_bytes=48 << 20, **options),
    )


def local(sizes, fields, coordinates, element_rank, element_slot):
    count = sizes[0] * sizes[1] * sizes[2]
    probes = element_slot.shape[0]
    elements = fields.shape[0]
    capacity = 5 * probes // (4 * count)
    blocks = -(-capacity // LANES)
    layout = jax.ShapeDtypeStruct((4 * blocks, count, LANES), F32)
    line = jax.ShapeDtypeStruct((1, probes), F32)

    lower = np.arange(CHUNK)
    prefix = np.concatenate([lower[:, None] <= lower[None, :], np.ones((CHUNK, CHUNK))], axis=1)
    turned = fields.reshape(elements, 256, 8).transpose(1, 2, 0).reshape(256, 8 * elements)
    nodes = jnp.broadcast_to(jnp.asarray(node_table, F32), (64, LANES))
    picker = pltpu.VMEM((8 * elements, GROUP * LANES), BF16)
    buffer = pltpu.VMEM(layout.shape, F32)
    arrivals = pltpu.SemaphoreType.DMA((count,))
    returned, row, lane = call(
        functools.partial(sample_kernel, sizes, blocks),
        6,
        (layout, line, line),
        [pltpu.VMEM((2 * count * blocks, 4 * LANES), F32)]
        + [buffer] * 3
        + [picker] * 2
        + [arrivals] * 4
        + [pltpu.SemaphoreType.DMA((2,))],
        collective_id=0,
        has_side_effects=True,
    )(
        element_rank.reshape(1, probes),
        coordinates,
        element_slot.reshape(1, probes),
        jnp.asarray(prefix, BF16),
        turned,
        nodes,
    )
    return call(
        functools.partial(return_kernel, blocks),
        3,
        jax.ShapeDtypeStruct((4, probes), F32),
        [pltpu.VMEM((4 * LANES, count * blocks), BF16)],
    )(returned, row, lane)


def solution(mesh):
    sizes = tuple(mesh.shape[axis] for axis in AXES)
    placed = (P(AXES, None), P(None, AXES), P(AXES, None), P(AXES))
    return jax.shard_map(
        functools.partial(local, sizes),
        mesh=mesh,
        in_specs=placed,
        out_specs=P(None, AXES),
        check_vma=False,
    )
```
